32 devices in a mesh: groups: 2 (over y), dom: 4 (over z), shot: 4 (over x, core).
Axes of the slice: x: 2, y: 2, z: 4, core: 2. Of those that a mesh axis runs over, the one named last changes fastest.
Arguments:
- courant_sq: float32 [128, 128, 128], P(('groups', 'dom')), parts along dimension 0, may hold values from 0.05 to 0.19
- adjoint_init: float32 [8, 2, 64, 128, 128], P(('groups', 'shot'), None, 'dom'), parts along dimension 0, may hold values from -6 to 6
- forward_saved: bfloat16 [8, 6, 64, 128, 128], P(('groups', 'shot'), None, 'dom'), parts along dimension 0, may hold values from -4 to 4
- residual_traces: float32 [8, 4, 1024], P(('groups', 'shot')), parts along dimension 0, may hold values from -6 to 6
- receivers: int32 [8, 1024, 3], P(('groups', 'shot')), parts along dimension 0, may hold values from 0 to 127, as said below
- sources: int32 [8, 3], P(('groups', 'shot')), parts along dimension 0, may hold values from 0 to 127, as said below
Outputs:
- gradient: float32 [128, 128, 128], P(('groups', 'dom'), 'shot'), parts along dimension 0
- adjoint_final: float32 [8, 2, 64, 128, 128], P(('groups', 'shot'), None, 'dom'), parts along dimension 0
The draws below stay inside these ranges and needn't reach their ends.
There are 2 independent parts, one for each index of `groups`. The reference program is written for one: setup_inputs(seed, part) draws one part's arguments, and reference() takes and returns one part's arrays. A program takes and returns all parts, laid end to end along the dimension named above; each array names one. Nothing has to cross between parts.
Inputs may be any that keep to these rules, and one draw needn't show every extreme that they name: Each row holds the depth index (below 64), the first horizontal index (below 128) and the second (below 128) of a cell; receivers may share cells. `sources`: each row holds the depth index (below 64), the first horizontal index (below 128) and the second (below 128) of a cell.
All inputs are finite; a program needn't handle non-finite values.
Results may differ from the reference program's by a relative error of at most 0.0003.
Values sent between devices are 32-bit elements; how exact they have to be, the bound alone decides.
A program may use at most 64 MiB of HBM per device.

```python
import jax
import jax.numpy as jnp

NX = 128
NY = 128
REC = 1024
ITERS = 4
RADIUS = 6
NZ = 64
SHOTS = 4


def draw_courant_sq(key, part):
    shape = (NZ, NX, NY)
    values = jax.random.uniform(jax.random.fold_in(key, 31), shape, jnp.float32, 0.05, 0.19)
    return values


def draw_adjoint_init(key, part):
    shape = (SHOTS, 2, NZ, NX, NY)
    rough = jax.random.normal(jax.random.fold_in(key, 47), shape, jnp.float32)
    values = jnp.clip(rough, -6.0, 6.0)
    return values


def draw_receivers(key, part):
    limits = jnp.array([NZ, NX, NY], jnp.int32)
    return jax.random.randint(jax.random.fold_in(key, 11), (SHOTS, REC, 3), 0, limits).astype(jnp.int32)


def draw_sources(key, part):
    limits = jnp.array([NZ, NX, NY], jnp.int32)
    values = jax.random.randint(jax.random.fold_in(key, 23), (SHOTS, 3), 0, limits).astype(jnp.int32)
    if NZ >= max(NX, NY):
        values = values.at[0, 0].set(NZ - 1)
    elif NX >= NY:
        values = values.at[0, 1].set(NX - 1)
    else:
        values = values.at[0, 2].set(NY - 1)
    values = values.at[1, 1].set(0)
    return values.astype(jnp.int32)


def block_scale(own_key, extent, pieces, smallest, top_value):
    loudness = 1.0
    for position, blocks in pieces:
        draws = jax.random.uniform(jax.random.fold_in(jax.random.fold_in(own_key, 6), position), (blocks,), jnp.float32, smallest / len(pieces), top_value / len(pieces))
        loudness = loudness * jnp.repeat(jnp.exp(draws), extent[position] // blocks).reshape((-1,) + (1,) * (len(extent) - 1 - position))
    return loudness


def centred(stream_key, dims, scale, bound, shards=(), kind=jnp.bfloat16):
    values = jax.random.normal(stream_key, dims, jnp.float32) * scale
    if len(shards) > 0:
        values = block_scale(stream_key, dims, shards, -0.22, 0.18) * values
    return jnp.clip(values, min=-bound, max=bound).astype(kind)


def setup_inputs(seed: int = 0, part: int = 0) -> dict:
    streams_of = jax.random.split(jax.random.key(seed), 7)
    own_keys = jax.random.split(jax.random.fold_in(streams_of[6], part), 7)
    courant_sq = draw_courant_sq(jax.random.fold_in(jax.random.fold_in(streams_of[6], part), 71), part)
    adjoint_init = draw_adjoint_init(jax.random.fold_in(jax.random.fold_in(streams_of[6], part), 71), part)
    forward_saved = centred(own_keys[2], (SHOTS, ITERS + 2, NZ, NX, NY), 0.25, 4.0, ((0, 4), (2, 4)))
    residual_traces = centred(own_keys[3], (SHOTS, ITERS, REC), 1.0, 6.0, ((0, 4),), jnp.float32)
    receivers = draw_receivers(jax.random.fold_in(jax.random.fold_in(streams_of[6], part), 71), part)
    sources = draw_sources(jax.random.fold_in(jax.random.fold_in(streams_of[6], part), 71), part)
    return {"courant_sq": courant_sq, "adjoint_init": adjoint_init, "forward_saved": forward_saved, "residual_traces": residual_traces, "receivers": receivers, "sources": sources}


STENCIL_WEIGHTS = (-205.0 / 72.0, 8.0 / 5.0, -1.0 / 5.0, 8.0 / 315.0, -1.0 / 560.0)


def laplacian(field):
    size_z, size_x, size_y = field.shape
    padded = jnp.pad(field, 4)
    center = padded[4:4 + size_z, 4:4 + size_x, 4:4 + size_y]
    summed = 3.0 * STENCIL_WEIGHTS[0] * center
    for offset in range(1, 5):
        beside_all = padded[4 + offset:4 + offset + size_z, 4:4 + size_x, 4:4 + size_y]
        beside_all = beside_all + padded[4 - offset:4 - offset + size_z, 4:4 + size_x, 4:4 + size_y]
        beside_all = beside_all + padded[4:4 + size_z, 4 + offset:4 + offset + size_x, 4:4 + size_y]
        beside_all = beside_all + padded[4:4 + size_z, 4 - offset:4 - offset + size_x, 4:4 + size_y]
        beside_all = beside_all + padded[4:4 + size_z, 4:4 + size_x, 4 + offset:4 + offset + size_y]
        beside_all = beside_all + padded[4:4 + size_z, 4:4 + size_x, 4 - offset:4 - offset + size_y]
        summed = summed + STENCIL_WEIGHTS[offset] * beside_all
    return summed


def source_taper(source, depth_first, size_z, size_x, size_y):
    depth_gap = jnp.arange(size_z, dtype=jnp.int32) + depth_first - source[0]
    across_gap = jnp.arange(size_x, dtype=jnp.int32) - source[1]
    along_gap = jnp.arange(size_y, dtype=jnp.int32) - source[2]
    distance = (depth_gap * depth_gap)[:, None, None] + (across_gap * across_gap)[None, :, None] + (along_gap * along_gap)[None, None, :]
    return 1.0 - jnp.exp(-distance.astype(jnp.float32) / float(RADIUS * RADIUS))


def reference(courant_sq, adjoint_init, forward_saved, residual_traces, receivers, sources):
    size_z, size_x, size_y = courant_sq.shape
    gradient = jnp.zeros((size_z, size_x, size_y), jnp.float32)
    finals = []
    for shot_index in range(SHOTS):
        level_later = adjoint_init[shot_index, 0]
        level_now = adjoint_init[shot_index, 1]
        spots = receivers[shot_index]
        summed = jnp.zeros((size_z, size_x, size_y), jnp.float32)
        for section in range(ITERS - 1, -1, -1):
            level_next = 2.0 * level_now - level_later + courant_sq * laplacian(level_now)
            level_next = level_next.at[spots[:, 0], spots[:, 1], spots[:, 2]].add(residual_traces[shot_index, section])
            forward_accel = forward_saved[shot_index, section + 2].astype(jnp.float32) - 2.0 * forward_saved[shot_index, section + 1].astype(jnp.float32) + forward_saved[shot_index, section].astype(jnp.float32)
            summed = summed + level_next * forward_accel
            level_later, level_now = level_now, level_next
        gradient = gradient + source_taper(sources[shot_index], 0, size_z, size_x, size_y) * summed
        finals.append(jnp.stack([level_later, level_now]))
    return gradient, jnp.stack(finals)
```

```python
import functools

import jax
import jax.numpy as jnp
from jax import lax
from jax.experimental import pallas as pl
from jax.experimental.pallas import tpu as pltpu
from jax.sharding import PartitionSpec as P

ITERS = 4
RADIUS = 6
HALO = 4
PAD = 8

STENCIL_WEIGHTS = (-205.0 / 72.0, 8.0 / 5.0, -1.0 / 5.0, 8.0 / 315.0, -1.0 / 560.0)


def kernel(
    dom_n,
    shot_n,
    source_ref,
    spot_ref,
    trace_ref,
    courant_hbm,
    init_hbm,
    fwd_hbm,
    grad_ref,
    final_hbm,
    lev,
    courant,
    fwd,
    image,
    hot,
    src,
    band,
    parts,
    in_sem,
    send_sem,
    recv_sem,
    part_send,
    part_recv,
    out_sem,
):
    slab, size_x, size_y = courant.shape
    rows = size_x // shot_n
    me = lax.axis_index("dom")
    shot = lax.axis_index("shot")
    has_up = me > 0
    has_down = me < dom_n - 1

    loads = [
        pltpu.make_async_copy(
            init_hbm.at[1], lev.at[1, pl.ds(HALO, slab), pl.ds(PAD, size_x), :], in_sem.at[0]
        ),
        pltpu.make_async_copy(
            init_hbm.at[0], lev.at[0, pl.ds(HALO, slab), pl.ds(PAD, size_x), :], in_sem.at[1]
        ),
        pltpu.make_async_copy(courant_hbm, courant, in_sem.at[2]),
        pltpu.make_async_copy(fwd_hbm, fwd, in_sem.at[3]),
    ]
    for load in loads:
        load.start()

    @pl.when(jnp.logical_not(has_up))
    def _():
        for level in range(1, ITERS + 1):
            lev[level, 0:HALO] = jnp.zeros((HALO, size_x + 2 * PAD, size_y), jnp.float32)

    @pl.when(jnp.logical_not(has_down))
    def _():
        for level in range(1, ITERS + 1):
            lev[level, HALO + slab :] = jnp.zeros((HALO, size_x + 2 * PAD, size_y), jnp.float32)

    barrier = pltpu.get_barrier_semaphore()

    @pl.when(has_up)
    def _():
        pl.semaphore_signal(barrier, inc=1, device_id={"dom": me - 1})

    @pl.when(has_down)
    def _():
        pl.semaphore_signal(barrier, inc=1, device_id={"dom": me + 1})

    for d in range(1, shot_n):
        pl.semaphore_signal(barrier, inc=1, device_id={"shot": lax.rem(shot + d, shot_n)})
    pl.semaphore_wait(
        barrier, has_up.astype(jnp.int32) + has_down.astype(jnp.int32) + (shot_n - 1)
    )

    def halo_copies(step, strip):
        level = step + 1
        cut = pl.ds(PAD + strip * rows, rows)
        if step == 0:
            plain = pl.ds(strip * rows, rows)
            low = init_hbm.at[1, pl.ds(0, HALO), plain, :]
            high = init_hbm.at[1, pl.ds(slab - HALO, HALO), plain, :]
        else:
            low = lev.at[level, pl.ds(HALO, HALO), cut, :]
            high = lev.at[level, pl.ds(slab, HALO), cut, :]
        upward = pltpu.make_async_remote_copy(
            src_ref=low,
            dst_ref=lev.at[level, pl.ds(HALO + slab, HALO), cut, :],
            send_sem=send_sem.at[step, 0, strip],
            recv_sem=recv_sem.at[step, 0, strip],
            device_id={"dom": me - 1},
        )
        downward = pltpu.make_async_remote_copy(
            src_ref=high,
            dst_ref=lev.at[level, pl.ds(0, HALO), cut, :],
            send_sem=send_sem.at[step, 1, strip],
            recv_sem=recv_sem.at[step, 1, strip],
            device_id={"dom": me + 1},
        )
        return upward, downward

    def send_halo(step, strip):
        upward, downward = halo_copies(step, strip)

        @pl.when(has_up)
        def _():
            upward.start()

        @pl.when(has_down)
        def _():
            downward.start()

    def wait_halo(step, strip):
        upward, downward = halo_copies(step, strip)

        @pl.when(has_down)
        def _():
            upward.wait_recv()

        @pl.when(has_up)
        def _():
            downward.wait_recv()

    def wait_sent(step, strip):
        upward, downward = halo_copies(step, strip)

        @pl.when(has_up)
        def _():
            upward.wait_send()

        @pl.when(has_down)
        def _():
            downward.wait_send()

    for strip in range(shot_n):
        send_halo(0, strip)

    for level in range(1, ITERS + 1):
        lev[level, HALO : HALO + slab, 0:PAD] = jnp.zeros((slab, PAD, size_y), jnp.float32)
        lev[level, HALO : HALO + slab, PAD + size_x :] = jnp.zeros(
            (slab, PAD, size_y), jnp.float32
        )
    gap = jnp.abs(
        lax.broadcasted_iota(jnp.int32, (size_y, size_y), 0)
        - lax.broadcasted_iota(jnp.int32, (size_y, size_y), 1)
    )
    weights = jnp.where(gap == 0, jnp.float32(3.0 * STENCIL_WEIGHTS[0]), jnp.float32(0.0))
    for offset in range(1, HALO + 1):
        weights = jnp.where(gap == offset, jnp.float32(STENCIL_WEIGHTS[offset]), weights)
    band[...] = weights

    n_rec = spot_ref.shape[1]

    @pl.loop(0, slab)
    def _(z):
        row = lax.broadcasted_iota(jnp.int32, (size_x, n_rec), 0) + z * size_x
        same = row == spot_ref[0:1, :]
        hot[pl.ds(pl.multiple_of(z * size_x, size_x), size_x), :] = jnp.where(
            same, 1.0, 0.0
        ).astype(jnp.bfloat16)

    def place(section):
        amount = trace_ref[section : section + 1, :]
        high = amount.astype(jnp.bfloat16).astype(jnp.float32)
        low = amount - high
        same = lax.broadcasted_iota(jnp.int32, (size_y, n_rec), 0) == spot_ref[1:2, :]
        columns = jnp.concatenate(
            [jnp.where(same, high, 0.0), jnp.where(same, low, 0.0)], axis=0
        ).astype(jnp.bfloat16)
        block = 4 * size_x

        @pl.loop(0, slab * size_x // block)
        def _(i):
            cut = pl.ds(pl.multiple_of(i * block, block), block)
            src[cut, :] = lax.dot_general(
                hot[cut, :],
                columns,
                (((1,), (1,)), ((), ())),
                preferred_element_type=jnp.float32,
            )

    def update(step, z, planes, first, count):
        level = step + 1
        section = ITERS - 1 - step
        cut = pl.ds(PAD + first, count)
        plain = pl.ds(first, count)
        here = pl.ds(z, planes)
        now = lev[level, pl.ds(HALO + z, planes), cut, :]
        total = lax.dot_general(
            now.reshape(planes * count, size_y),
            band[...],
            (((1,), (0,)), ((), ())),
            precision=lax.Precision.HIGHEST,
            preferred_element_type=jnp.float32,
        ).reshape(planes, count, size_y)
        for offset in range(1, HALO + 1):
            beside = (
                lev[level, pl.ds(HALO + z + offset, planes), cut, :]
                + lev[level, pl.ds(HALO + z - offset, planes), cut, :]
                + lev[level, pl.ds(HALO + z, planes), pl.ds(PAD + first + offset, count), :]
                + lev[level, pl.ds(HALO + z, planes), pl.ds(PAD + first - offset, count), :]
            )
            total = total + STENCIL_WEIGHTS[offset] * beside
        added = []
        for p in range(planes):
            at = pl.ds(pl.multiple_of((z + p) * size_x + first, 8), count)
            added.append(src[at, 0:size_y] + src[at, size_y : 2 * size_y])
        added = added[0][None] if planes == 1 else jnp.stack(added)
        later = lev[level - 1, pl.ds(HALO + z, planes), cut, :]
        new = 2.0 * now - later + courant[here, plain, :] * total + added
        lev[level + 1, pl.ds(HALO + z, planes), cut, :] = new
        accel = (
            fwd[section + 2, here, plain, :].astype(jnp.float32)
            - 2.0 * fwd[section + 1, here, plain, :].astype(jnp.float32)
            + fwd[section, here, plain, :].astype(jnp.float32)
        )
        value = new * accel
        if step > 0:
            value = value + image[here, plain, :]
        if step == ITERS - 1:
            shape = (planes, count, size_y)
            dz = lax.broadcasted_iota(jnp.int32, shape, 0) + (me * slab + z - source_ref[0])
            dx = lax.broadcasted_iota(jnp.int32, shape, 1) + (first - source_ref[1])
            dy = lax.broadcasted_iota(jnp.int32, shape, 2) - source_ref[2]
            distance = (dz * dz + dx * dx + dy * dy).astype(jnp.float32)
            value = value * (1.0 - jnp.exp(distance * (-1.0 / float(RADIUS * RADIUS))))
        image[here, plain, :] = value

    def part_copy(d, group, first_z, planes):
        target = lax.rem(shot + d, shot_n)
        return pltpu.make_async_remote_copy(
            src_ref=image.at[
                pl.ds(first_z, planes), pl.ds(pl.multiple_of(target * rows, 8), rows), :
            ],
            dst_ref=parts.at[d - 1, pl.ds(first_z, planes), :, :],
            send_sem=part_send.at[group, d - 1],
            recv_sem=part_recv.at[group, d - 1],
            device_id={"shot": target},
        )

    groups = ((HALO, slab - 2 * HALO), (0, HALO), (slab - HALO, HALO))

    def final_copy(index, group):
        first_z, planes = groups[group]
        return pltpu.make_async_copy(
            lev.at[ITERS + index, pl.ds(HALO + first_z, planes), pl.ds(PAD, size_x), :],
            final_hbm.at[index, pl.ds(first_z, planes)],
            out_sem.at[index, group],
        )

    for step in range(ITERS):
        last = step == ITERS - 1
        place(ITERS - 1 - step)
        if step == 0:
            for load in loads:
                load.wait()

        @pl.loop(HALO, slab - HALO)
        def _(z):
            update(step, z, 1, 0, size_x)

        if last:
            final_copy(1, 0).start()
            for d in range(1, shot_n):
                part_copy(d, 0, *groups[0]).start()

        for strip in range(shot_n):
            wait_halo(step, strip)
            update(step, 0, HALO, strip * rows, rows)
            update(step, slab - HALO, HALO, strip * rows, rows)
            if not last:
                send_halo(step + 1, strip)

        if step == ITERS - 2:
            for group in range(3):
                final_copy(0, group).start()

    for group in (1, 2):
        final_copy(1, group).start()
        for d in range(1, shot_n):
            part_copy(d, group, *groups[group]).start()

    for group in range(3):
        first_z, planes = groups[group]
        value = image[
            first_z : first_z + planes, pl.ds(pl.multiple_of(shot * rows, 8), rows), :
        ]
        for d in range(1, shot_n):
            part_copy(d, group, first_z, planes).wait_recv()
            value = value + parts[d - 1, first_z : first_z + planes]
        grad_ref[first_z : first_z + planes] = value

    for step in range(ITERS):
        for strip in range(shot_n):
            wait_sent(step, strip)
    for group in range(3):
        for d in range(1, shot_n):
            part_copy(d, group, *groups[group]).wait_send()
        final_copy(0, group).wait()
        final_copy(1, group).wait()


def per_device(
    dom_n, shot_n, courant_sq, adjoint_init, forward_saved, residual_traces, receivers, sources
):
    slab, size_x, size_y = courant_sq.shape
    n_rec = receivers.shape[1]
    first_row = lax.axis_index("dom") * slab
    spots = receivers[0]
    spot_rows = (spots[:, 0] - first_row) * size_x + spots[:, 1]
    spot = jnp.stack([spot_rows, spots[:, 2]])
    hbm = pl.BlockSpec(memory_space=pl.ANY)
    vmem = pl.BlockSpec(memory_space=pltpu.VMEM)
    gradient, final = pl.pallas_call(
        functools.partial(kernel, dom_n, shot_n),
        out_shape=(
            jax.ShapeDtypeStruct((slab, size_x // shot_n, size_y), jnp.float32),
            jax.ShapeDtypeStruct((2, slab, size_x, size_y), jnp.float32),
        ),
        in_specs=[pl.BlockSpec(memory_space=pltpu.SMEM), vmem, vmem, hbm, hbm, hbm],
        out_specs=(vmem, hbm),
        scratch_shapes=[
            pltpu.VMEM((ITERS + 2, slab + 2 * HALO, size_x + 2 * PAD, size_y), jnp.float32),
            pltpu.VMEM((slab, size_x, size_y), jnp.float32),
            pltpu.VMEM((ITERS + 2, slab, size_x, size_y), jnp.bfloat16),
            pltpu.VMEM((slab, size_x, size_y), jnp.float32),
            pltpu.VMEM((slab * size_x, n_rec), jnp.bfloat16),
            pltpu.VMEM((slab * size_x, 2 * size_y), jnp.float32),
            pltpu.VMEM((size_y, size_y), jnp.float32),
            pltpu.VMEM((shot_n - 1, slab, size_x // shot_n, size_y), jnp.float32),
            pltpu.SemaphoreType.DMA((4,)),
            pltpu.SemaphoreType.DMA((ITERS, 2, shot_n)),
            pltpu.SemaphoreType.DMA((ITERS, 2, shot_n)),
            pltpu.SemaphoreType.DMA((3, shot_n - 1)),
            pltpu.SemaphoreType.DMA((3, shot_n - 1)),
            pltpu.SemaphoreType.DMA((2, 3)),
        ],
        compiler_params=pltpu.CompilerParams(
            collective_id=0, has_side_effects=True, vmem_limit_bytes=60 * 1024 * 1024
        ),
    )(
        sources[0],
        spot,
        residual_traces[0],
        courant_sq,
        adjoint_init[0],
        forward_saved[0],
    )
    return gradient, final[None]


def solution(mesh):
    placed = (
        P(("groups", "dom"), None, None),
        P(("groups", "shot"), None, "dom", None, None),
        P(("groups", "shot"), None, "dom", None, None),
        P(("groups", "shot"), None, None),
        P(("groups", "shot"), None, None),
        P(("groups", "shot"), None),
    )
    return jax.shard_map(
        functools.partial(per_device, mesh.shape["dom"], mesh.shape["shot"]),
        mesh=mesh,
        in_specs=placed,
        out_specs=(
            P(("groups", "dom"), "shot", None),
            P(("groups", "shot"), None, "dom", None, None),
        ),
        check_vma=False,
    )
```

```python
import functools

import jax
import jax.numpy as jnp
from jax import lax
from jax.experimental import pallas as pl
from jax.experimental.pallas import tpu as pltpu
from jax.sharding import PartitionSpec as P

ITERS = 4
RADIUS = 6
HALO = 4
PAD = 8

STENCIL_WEIGHTS = (-205.0 / 72.0, 8.0 / 5.0, -1.0 / 5.0, 8.0 / 315.0, -1.0 / 560.0)


def kernel(
    dom_n,
    shot_n,
    source_ref,
    spot_ref,
    trace_ref,
    courant_hbm,
    init_hbm,
    fwd_hbm,
    grad_ref,
    final_ref,
    lev,
    courant,
    fwd,
    image,
    hot,
    src,
    band,
    parts,
    in_sem,
    send_sem,
    recv_sem,
    part_send,
    part_recv,
):
    slab, size_x, size_y = courant.shape
    rows = size_x // shot_n
    me = lax.axis_index("dom")
    shot = lax.axis_index("shot")
    has_up = me > 0
    has_down = me < dom_n - 1

    loads = [
        pltpu.make_async_copy(
            init_hbm.at[1], lev.at[1, pl.ds(HALO, slab), pl.ds(PAD, size_x), :], in_sem.at[0]
        ),
        pltpu.make_async_copy(
            init_hbm.at[0], lev.at[0, pl.ds(HALO, slab), pl.ds(PAD, size_x), :], in_sem.at[1]
        ),
        pltpu.make_async_copy(courant_hbm, courant, in_sem.at[2]),
        pltpu.make_async_copy(fwd_hbm, fwd, in_sem.at[3]),
    ]
    for load in loads:
        load.start()

    @pl.when(jnp.logical_not(has_up))
    def _():
        for level in range(1, ITERS + 1):
            lev[level, 0:HALO] = jnp.zeros((HALO, size_x + 2 * PAD, size_y), jnp.float32)

    @pl.when(jnp.logical_not(has_down))
    def _():
        for level in range(1, ITERS + 1):
            lev[level, HALO + slab :] = jnp.zeros((HALO, size_x + 2 * PAD, size_y), jnp.float32)

    barrier = pltpu.get_barrier_semaphore()

    @pl.when(has_up)
    def _():
        pl.semaphore_signal(barrier, inc=1, device_id={"dom": me - 1})

    @pl.when(has_down)
    def _():
        pl.semaphore_signal(barrier, inc=1, device_id={"dom": me + 1})

    for d in range(1, shot_n):
        pl.semaphore_signal(barrier, inc=1, device_id={"shot": lax.rem(shot + d, shot_n)})
    pl.semaphore_wait(
        barrier, has_up.astype(jnp.int32) + has_down.astype(jnp.int32) + (shot_n - 1)
    )

    def owner(i):
        i = i + 1
        if shot_n % 2:
            return lax.rem(shot + i, shot_n)
        pair = lax.rem(lax.div(shot, 2) + (i // 2 + i % 2) % (shot_n // 2), shot_n // 2)
        return pair * 2 + lax.rem(shot + i, 2)

    def halo_copies(step, strip):
        level = step + 1
        begin = pl.multiple_of(owner(strip) * rows, 8)
        cut = pl.ds(pl.multiple_of(PAD + begin, 8), rows)
        if step == 0:
            plain = pl.ds(begin, rows)
            low = init_hbm.at[1, pl.ds(0, HALO), plain, :]
            high = init_hbm.at[1, pl.ds(slab - HALO, HALO), plain, :]
        else:
            low = lev.at[level, pl.ds(HALO, HALO), cut, :]
            high = lev.at[level, pl.ds(slab, HALO), cut, :]
        upward = pltpu.make_async_remote_copy(
            src_ref=low,
            dst_ref=lev.at[level, pl.ds(HALO + slab, HALO), cut, :],
            send_sem=send_sem.at[step, 0, strip],
            recv_sem=recv_sem.at[step, 0, strip],
            device_id={"dom": me - 1},
        )
        downward = pltpu.make_async_remote_copy(
            src_ref=high,
            dst_ref=lev.at[level, pl.ds(0, HALO), cut, :],
            send_sem=send_sem.at[step, 1, strip],
            recv_sem=recv_sem.at[step, 1, strip],
            device_id={"dom": me + 1},
        )
        return upward, downward

    def send_halo(step, strip):
        upward, downward = halo_copies(step, strip)

        @pl.when(has_up)
        def _():
            upward.start()

        @pl.when(has_down)
        def _():
            downward.start()

    def wait_halo(step, strip):
        upward, downward = halo_copies(step, strip)

        @pl.when(has_down)
        def _():
            upward.wait_recv()

        @pl.when(has_up)
        def _():
            downward.wait_recv()

    def wait_sent(step, strip):
        upward, downward = halo_copies(step, strip)

        @pl.when(has_up)
        def _():
            upward.wait_send()

        @pl.when(has_down)
        def _():
            downward.wait_send()

    for strip in range(shot_n):
        send_halo(0, strip)

    for level in range(1, ITERS + 1):
        lev[level, HALO : HALO + slab, 0:PAD] = jnp.zeros((slab, PAD, size_y), jnp.float32)
        lev[level, HALO : HALO + slab, PAD + size_x :] = jnp.zeros(
            (slab, PAD, size_y), jnp.float32
        )
    gap = jnp.abs(
        lax.broadcasted_iota(jnp.int32, (size_y, size_y), 0)
        - lax.broadcasted_iota(jnp.int32, (size_y, size_y), 1)
    )
    weights = jnp.where(gap == 0, jnp.float32(3.0 * STENCIL_WEIGHTS[0]), jnp.float32(0.0))
    for offset in range(1, HALO + 1):
        weights = jnp.where(gap == offset, jnp.float32(STENCIL_WEIGHTS[offset]), weights)
    band[...] = weights

    n_rec = spot_ref.shape[2]

    @pl.loop(0, slab)
    def _(z):
        row = lax.broadcasted_iota(jnp.int32, (size_x, n_rec), 0) + z * size_x
        same = row == (spot_ref[0] - me * slab) * size_x + spot_ref[1]
        hot[pl.ds(pl.multiple_of(z * size_x, size_x), size_x), :] = jnp.where(
            same, 1.0, 0.0
        ).astype(jnp.bfloat16)

    def place(section):
        amount = trace_ref[section : section + 1, :]
        high = amount.astype(jnp.bfloat16).astype(jnp.float32)
        low = amount - high
        same = lax.broadcasted_iota(jnp.int32, (size_y, n_rec), 0) == spot_ref[2]
        columns = jnp.concatenate(
            [jnp.where(same, high, 0.0), jnp.where(same, low, 0.0)], axis=0
        ).astype(jnp.bfloat16)
        block = 4 * size_x

        @pl.loop(0, slab * size_x // block)
        def _(i):
            cut = pl.ds(pl.multiple_of(i * block, block), block)
            src[cut, :] = lax.dot_general(
                hot[cut, :],
                columns,
                (((1,), (1,)), ((), ())),
                preferred_element_type=jnp.float32,
            )

    def update(step, z, planes, first, count):
        level = step + 1
        section = ITERS - 1 - step
        cut = pl.ds(PAD + first, count)
        plain = pl.ds(first, count)
        here = pl.ds(z, planes)
        now = lev[level, pl.ds(HALO + z, planes), cut, :]
        total = lax.dot_general(
            now.reshape(planes * count, size_y),
            band[...],
            (((1,), (0,)), ((), ())),
            precision=lax.Precision.HIGHEST,
            preferred_element_type=jnp.float32,
        ).reshape(planes, count, size_y)
        for offset in range(1, HALO + 1):
            beside = (
                lev[level, pl.ds(HALO + z + offset, planes), cut, :]
                + lev[level, pl.ds(HALO + z - offset, planes), cut, :]
                + lev[level, pl.ds(HALO + z, planes), pl.ds(PAD + first + offset, count), :]
                + lev[level, pl.ds(HALO + z, planes), pl.ds(PAD + first - offset, count), :]
            )
            total = total + STENCIL_WEIGHTS[offset] * beside
        added = []
        for p in range(planes):
            at = pl.ds(pl.multiple_of((z + p) * size_x + first, 8), count)
            added.append(src[at, 0:size_y] + src[at, size_y : 2 * size_y])
        added = added[0][None] if planes == 1 else jnp.stack(added)
        later = lev[level - 1, pl.ds(HALO + z, planes), cut, :]
        new = 2.0 * now - later + courant[here, plain, :] * total + added
        if step < ITERS - 1:
            lev[level + 1, pl.ds(HALO + z, planes), cut, :] = new
        if step >= ITERS - 2:
            final_ref[step - (ITERS - 2), here, plain, :] = new
        accel = (
            fwd[section + 2, here, plain, :].astype(jnp.float32)
            - 2.0 * fwd[section + 1, here, plain, :].astype(jnp.float32)
            + fwd[section, here, plain, :].astype(jnp.float32)
        )
        value = new * accel
        if step > 0:
            value = value + image[here, plain, :]
        if step == ITERS - 1:
            shape = (planes, count, size_y)
            dz = lax.broadcasted_iota(jnp.int32, shape, 0) + (me * slab + z - source_ref[0])
            dx = lax.broadcasted_iota(jnp.int32, shape, 1) + (first - source_ref[1])
            dy = lax.broadcasted_iota(jnp.int32, shape, 2) - source_ref[2]
            distance = (dz * dz + dx * dx + dy * dy).astype(jnp.float32)
            value = value * (1.0 - jnp.exp(distance * (-1.0 / float(RADIUS * RADIUS))))
        image[here, plain, :] = value

    def part_copy(i, group):
        first_z, planes = groups[group]
        return pltpu.make_async_remote_copy(
            src_ref=image.at[
                pl.ds(first_z, planes), pl.ds(pl.multiple_of(owner(i) * rows, 8), rows), :
            ],
            dst_ref=parts.at[i, pl.ds(first_z, planes), :, :],
            send_sem=part_send.at[group, i],
            recv_sem=part_recv.at[group, i],
            device_id={"shot": owner(i)},
        )

    groups = ((HALO, slab - 2 * HALO), (0, HALO), (slab - HALO, HALO))

    for step in range(ITERS):
        last = step == ITERS - 1
        place(ITERS - 1 - step)
        if step == 0:
            for load in loads:
                load.wait()

        @pl.loop(HALO, slab - HALO)
        def _(z):
            update(step, z, 1, 0, size_x)

        if last:
            for i in range(shot_n - 1):
                part_copy(i, 0).start()

        for i in range(shot_n):
            first = pl.multiple_of(owner(i) * rows, 8)
            wait_halo(step, i)
            update(step, 0, HALO, first, rows)
            update(step, slab - HALO, HALO, first, rows)
            if not last:
                send_halo(step + 1, i)
            elif i < shot_n - 1:
                part_copy(i, 1).start()
                part_copy(i, 2).start()

    mine = pl.ds(pl.multiple_of(shot * rows, 8), rows)
    for group in range(3):
        first_z, planes = groups[group]
        value = image[first_z : first_z + planes, mine, :]
        for i in range(shot_n - 1):
            part_copy(i, group).wait_recv()
            value = value + parts[i, first_z : first_z + planes]
        grad_ref[first_z : first_z + planes] = value

    for step in range(ITERS):
        for i in range(shot_n):
            wait_sent(step, i)
    for group in range(3):
        for i in range(shot_n - 1):
            part_copy(i, group).wait_send()


def per_device(
    dom_n, shot_n, courant_sq, adjoint_init, forward_saved, residual_traces, receivers, sources
):
    slab, size_x, size_y = courant_sq.shape
    n_rec = receivers.shape[1]
    spot = jnp.transpose(receivers, (2, 0, 1))
    hbm = pl.BlockSpec(memory_space=pl.ANY)
    vmem = pl.BlockSpec(memory_space=pltpu.VMEM)
    gradient, final = pl.pallas_call(
        functools.partial(kernel, dom_n, shot_n),
        out_shape=(
            pltpu.VMEM((slab, size_x // shot_n, size_y), jnp.float32),
            pltpu.VMEM((2, slab, size_x, size_y), jnp.float32),
        ),
        in_specs=[pl.BlockSpec(memory_space=pltpu.SMEM), vmem, vmem, hbm, hbm, hbm],
        out_specs=(vmem, vmem),
        scratch_shapes=[
            pltpu.VMEM((ITERS + 2, slab + 2 * HALO, size_x + 2 * PAD, size_y), jnp.float32),
            pltpu.VMEM((slab, size_x, size_y), jnp.float32),
            pltpu.VMEM((ITERS + 2, slab, size_x, size_y), jnp.bfloat16),
            pltpu.VMEM((slab, size_x, size_y), jnp.float32),
            pltpu.VMEM((slab * size_x, n_rec), jnp.bfloat16),
            pltpu.VMEM((slab * size_x, 2 * size_y), jnp.float32),
            pltpu.VMEM((size_y, size_y), jnp.float32),
            pltpu.VMEM((shot_n - 1, slab, size_x // shot_n, size_y), jnp.float32),
            pltpu.SemaphoreType.DMA((4,)),
            pltpu.SemaphoreType.DMA((ITERS, 2, shot_n)),
            pltpu.SemaphoreType.DMA((ITERS, 2, shot_n)),
            pltpu.SemaphoreType.DMA((3, shot_n - 1)),
            pltpu.SemaphoreType.DMA((3, shot_n - 1)),
        ],
        compiler_params=pltpu.CompilerParams(
            collective_id=0, has_side_effects=True, vmem_limit_bytes=60 * 1024 * 1024
        ),
    )(
        sources[0],
        spot,
        residual_traces[0],
        courant_sq,
        adjoint_init[0],
        forward_saved[0],
    )
    return gradient, final[None]


def solution(mesh):
    placed = (
        P(("groups", "dom"), None, None),
        P(("groups", "shot"), None, "dom", None, None),
        P(("groups", "shot"), None, "dom", None, None),
        P(("groups", "shot"), None, None),
        P(("groups", "shot"), None, None),
        P(("groups", "shot"), None),
    )
    return jax.shard_map(
        functools.partial(per_device, mesh.shape["dom"], mesh.shape["shot"]),
        mesh=mesh,
        in_specs=placed,
        out_specs=(
            P(("groups", "dom"), "shot", None),
            P(("groups", "shot"), None, "dom", None, None),
        ),
        check_vma=False,
    )
```

```python
import functools

import jax
import jax.numpy as jnp
from jax import lax
from jax.experimental import pallas as pl
from jax.experimental.pallas import tpu as pltpu
from jax.sharding import PartitionSpec as P

ITERS = 4
RADIUS = 6
HALO = 4
PAD = 8

STENCIL_WEIGHTS = (-205.0 / 72.0, 8.0 / 5.0, -1.0 / 5.0, 8.0 / 315.0, -1.0 / 560.0)


def kernel(
    dom_n,
    shot_n,
    source_ref,
    spot_ref,
    trace_ref,
    courant_hbm,
    init_hbm,
    fwd_hbm,
    grad_ref,
    final_ref,
    lev,
    courant,
    fwd,
    image,
    hot,
    src,
    band,
    parts,
    in_sem,
    send_sem,
    recv_sem,
    part_send,
    part_recv,
):
    slab, size_x, size_y = courant.shape
    rows = size_x // shot_n
    me = lax.axis_index("dom")
    shot = lax.axis_index("shot")
    has_up = me > 0
    has_down = me < dom_n - 1

    loads = [
        pltpu.make_async_copy(
            init_hbm.at[1], lev.at[1, pl.ds(HALO, slab), pl.ds(PAD, size_x), :], in_sem.at[0]
        ),
        pltpu.make_async_copy(
            init_hbm.at[0], lev.at[0, pl.ds(HALO, slab), pl.ds(PAD, size_x), :], in_sem.at[1]
        ),
        pltpu.make_async_copy(courant_hbm, courant, in_sem.at[2]),
        pltpu.make_async_copy(fwd_hbm, fwd, in_sem.at[3]),
    ]
    for load in loads:
        load.start()

    @pl.when(jnp.logical_not(has_up))
    def _():
        for level in range(1, ITERS + 1):
            lev[level, 0:HALO] = jnp.zeros((HALO, size_x + 2 * PAD, size_y), jnp.float32)

    @pl.when(jnp.logical_not(has_down))
    def _():
        for level in range(1, ITERS + 1):
            lev[level, HALO + slab :] = jnp.zeros((HALO, size_x + 2 * PAD, size_y), jnp.float32)

    barrier = pltpu.get_barrier_semaphore()

    @pl.when(has_up)
    def _():
        pl.semaphore_signal(barrier, inc=1, device_id={"dom": me - 1})

    @pl.when(has_down)
    def _():
        pl.semaphore_signal(barrier, inc=1, device_id={"dom": me + 1})

    for d in range(1, shot_n):
        pl.semaphore_signal(barrier, inc=1, device_id={"shot": lax.rem(shot + d, shot_n)})
    pl.semaphore_wait(
        barrier, has_up.astype(jnp.int32) + has_down.astype(jnp.int32) + (shot_n - 1)
    )

    def owner(i):
        i = i + 1
        if shot_n % 2:
            return lax.rem(shot + i, shot_n)
        pair = lax.rem(lax.div(shot, 2) + (i // 2 + i % 2) % (shot_n // 2), shot_n // 2)
        return pair * 2 + lax.rem(shot + i, 2)

    def halo_copies(step, strip):
        level = step + 1
        begin = pl.multiple_of(owner(strip) * rows, 8)
        cut = pl.ds(pl.multiple_of(PAD + begin, 8), rows)
        if step == 0:
            plain = pl.ds(begin, rows)
            low = init_hbm.at[1, pl.ds(0, HALO), plain, :]
            high = init_hbm.at[1, pl.ds(slab - HALO, HALO), plain, :]
        else:
            low = lev.at[level, pl.ds(HALO, HALO), cut, :]
            high = lev.at[level, pl.ds(slab, HALO), cut, :]
        upward = pltpu.make_async_remote_copy(
            src_ref=low,
            dst_ref=lev.at[level, pl.ds(HALO + slab, HALO), cut, :],
            send_sem=send_sem.at[step, 0, strip],
            recv_sem=recv_sem.at[step, 0, strip],
            device_id={"dom": me - 1},
        )
        downward = pltpu.make_async_remote_copy(
            src_ref=high,
            dst_ref=lev.at[level, pl.ds(0, HALO), cut, :],
            send_sem=send_sem.at[step, 1, strip],
            recv_sem=recv_sem.at[step, 1, strip],
            device_id={"dom": me + 1},
        )
        return upward, downward

    def send_halo(step, strip):
        upward, downward = halo_copies(step, strip)

        @pl.when(has_up)
        def _():
            upward.start()

        @pl.when(has_down)
        def _():
            downward.start()

    def wait_halo(step, strip):
        upward, downward = halo_copies(step, strip)

        @pl.when(has_down)
        def _():
            upward.wait_recv()

        @pl.when(has_up)
        def _():
            downward.wait_recv()

    def wait_sent(step, strip):
        upward, downward = halo_copies(step, strip)

        @pl.when(has_up)
        def _():
            upward.wait_send()

        @pl.when(has_down)
        def _():
            downward.wait_send()

    for strip in range(shot_n):
        send_halo(0, strip)

    for level in range(1, ITERS + 1):
        lev[level, HALO : HALO + slab, 0:PAD] = jnp.zeros((slab, PAD, size_y), jnp.float32)
        lev[level, HALO : HALO + slab, PAD + size_x :] = jnp.zeros(
            (slab, PAD, size_y), jnp.float32
        )
    gap = jnp.abs(
        lax.broadcasted_iota(jnp.int32, (size_y, size_y), 0)
        - lax.broadcasted_iota(jnp.int32, (size_y, size_y), 1)
    )
    weights = jnp.where(gap == 0, jnp.float32(3.0 * STENCIL_WEIGHTS[0]), jnp.float32(0.0))
    for offset in range(1, HALO + 1):
        weights = jnp.where(gap == offset, jnp.float32(STENCIL_WEIGHTS[offset]), weights)
    coarse = weights.astype(jnp.bfloat16)
    band[0:size_y, :] = coarse
    band[size_y : 2 * size_y, :] = coarse
    band[2 * size_y :, :] = (weights - coarse.astype(jnp.float32)).astype(jnp.bfloat16)

    n_rec = spot_ref.shape[2]

    @pl.loop(0, slab)
    def _(z):
        row = lax.broadcasted_iota(jnp.int32, (size_x, n_rec), 0) + z * size_x
        same = row == (spot_ref[0] - me * slab) * size_x + spot_ref[1]
        hot[pl.ds(pl.multiple_of(z * size_x, size_x), size_x), :] = jnp.where(
            same, 1.0, 0.0
        ).astype(jnp.bfloat16)

    def place(section):
        amount = trace_ref[section : section + 1, :]
        high = amount.astype(jnp.bfloat16).astype(jnp.float32)
        low = amount - high
        same = lax.broadcasted_iota(jnp.int32, (size_y, n_rec), 0) == spot_ref[2]
        columns = jnp.concatenate(
            [jnp.where(same, high, 0.0), jnp.where(same, low, 0.0)], axis=0
        ).astype(jnp.bfloat16)
        block = 4 * size_x

        @pl.loop(0, slab * size_x // block)
        def _(i):
            cut = pl.ds(pl.multiple_of(i * block, block), block)
            src[cut, :] = lax.dot_general(
                hot[cut, :],
                columns,
                (((1,), (1,)), ((), ())),
                preferred_element_type=jnp.float32,
            )

    def update(step, z, planes, first, count):
        level = step + 1
        section = ITERS - 1 - step
        cut = pl.ds(PAD + first, count)
        plain = pl.ds(first, count)
        here = pl.ds(z, planes)
        now = lev[level, pl.ds(HALO + z, planes), cut, :]
        flat = now.reshape(planes * count, size_y)
        high = flat.astype(jnp.bfloat16)
        low = (flat - high.astype(jnp.float32)).astype(jnp.bfloat16)
        total = lax.dot_general(
            jnp.concatenate([high, low, high], axis=1),
            band[...],
            (((1,), (0,)), ((), ())),
            preferred_element_type=jnp.float32,
        ).reshape(planes, count, size_y)
        for offset in range(1, HALO + 1):
            beside = (
                lev[level, pl.ds(HALO + z + offset, planes), cut, :]
                + lev[level, pl.ds(HALO + z - offset, planes), cut, :]
                + lev[level, pl.ds(HALO + z, planes), pl.ds(PAD + first + offset, count), :]
                + lev[level, pl.ds(HALO + z, planes), pl.ds(PAD + first - offset, count), :]
            )
            total = total + STENCIL_WEIGHTS[offset] * beside
        added = []
        for p in range(planes):
            at = pl.ds(pl.multiple_of((z + p) * size_x + first, 8), count)
            added.append(src[at, 0:size_y] + src[at, size_y : 2 * size_y])
        added = added[0][None] if planes == 1 else jnp.stack(added)
        later = lev[level - 1, pl.ds(HALO + z, planes), cut, :]
        new = 2.0 * now - later + courant[here, plain, :] * total + added
        if step < ITERS - 1:
            lev[level + 1, pl.ds(HALO + z, planes), cut, :] = new
        if step >= ITERS - 2:
            final_ref[step - (ITERS - 2), here, plain, :] = new
        accel = (
            fwd[section + 2, here, plain, :].astype(jnp.float32)
            - 2.0 * fwd[section + 1, here, plain, :].astype(jnp.float32)
            + fwd[section, here, plain, :].astype(jnp.float32)
        )
        value = new * accel
        if step > 0:
            value = value + image[here, plain, :]
        if step == ITERS - 1:
            shape = (planes, count, size_y)
            dz = lax.broadcasted_iota(jnp.int32, shape, 0) + (me * slab + z - source_ref[0])
            dx = lax.broadcasted_iota(jnp.int32, shape, 1) + (first - source_ref[1])
            dy = lax.broadcasted_iota(jnp.int32, shape, 2) - source_ref[2]
            distance = (dz * dz + dx * dx + dy * dy).astype(jnp.float32)
            value = value * (1.0 - jnp.exp(distance * (-1.0 / float(RADIUS * RADIUS))))
        image[here, plain, :] = value

    paired = shot_n == 4

    def part_copy(i, group):
        first_z, planes = groups[group]
        target = owner(2) if paired and i == 0 else owner(i)
        return pltpu.make_async_remote_copy(
            src_ref=image.at[
                pl.ds(first_z, planes), pl.ds(pl.multiple_of(owner(i) * rows, 8), rows), :
            ],
            dst_ref=parts.at[i, pl.ds(first_z, planes), :, :],
            send_sem=part_send.at[group, i],
            recv_sem=part_recv.at[group, i],
            device_id={"shot": target},
        )

    def part_start(i, group):
        if paired and i == 1:
            first_z, planes = groups[group]
            strip = pl.ds(pl.multiple_of(owner(1) * rows, 8), rows)
            part_copy(0, group).wait_recv()
            here = pl.ds(first_z, planes)
            image[here, strip, :] = image[here, strip, :] + parts[0, here]
        part_copy(i, group).start()

    groups = ((HALO, slab - 2 * HALO), (0, HALO), (slab - HALO, HALO))

    for step in range(ITERS):
        last = step == ITERS - 1
        place(ITERS - 1 - step)
        if step == 0:
            for load in loads:
                load.wait()

        @pl.loop(HALO, slab - HALO, step=HALO)
        def _(z):
            for strip in range(shot_n):
                update(step, z, HALO, strip * rows, rows)

        if last:
            for i in (0, 2, 1) if paired else range(shot_n - 1):
                part_start(i, 0)

        for i in range(shot_n):
            first = pl.multiple_of(owner(i) * rows, 8)
            wait_halo(step, i)
            update(step, 0, HALO, first, rows)
            update(step, slab - HALO, HALO, first, rows)
            if not last:
                send_halo(step + 1, i)
            elif i < shot_n - 1:
                part_start(i, 1)
                part_start(i, 2)

    mine = pl.ds(pl.multiple_of(shot * rows, 8), rows)
    for group in range(3):
        first_z, planes = groups[group]
        value = image[first_z : first_z + planes, mine, :]
        for i in (1, 2) if paired else range(shot_n - 1):
            part_copy(i, group).wait_recv()
            value = value + parts[i, first_z : first_z + planes]
        grad_ref[first_z : first_z + planes] = value

    for step in range(ITERS):
        for i in range(shot_n):
            wait_sent(step, i)
    for group in range(3):
        for i in range(shot_n - 1):
            part_copy(i, group).wait_send()


def per_device(
    dom_n, shot_n, courant_sq, adjoint_init, forward_saved, residual_traces, receivers, sources
):
    slab, size_x, size_y = courant_sq.shape
    n_rec = receivers.shape[1]
    spot = jnp.transpose(receivers, (2, 0, 1))
    hbm = pl.BlockSpec(memory_space=pl.ANY)
    vmem = pl.BlockSpec(memory_space=pltpu.VMEM)
    gradient, final = pl.pallas_call(
        functools.partial(kernel, dom_n, shot_n),
        out_shape=(
            pltpu.VMEM((slab, size_x // shot_n, size_y), jnp.float32),
            pltpu.VMEM((2, slab, size_x, size_y), jnp.float32),
        ),
        in_specs=[pl.BlockSpec(memory_space=pltpu.SMEM), vmem, vmem, hbm, hbm, hbm],
        out_specs=(vmem, vmem),
        scratch_shapes=[
            pltpu.VMEM((ITERS + 2, slab + 2 * HALO, size_x + 2 * PAD, size_y), jnp.float32),
            pltpu.VMEM((slab, size_x, size_y), jnp.float32),
            pltpu.VMEM((ITERS + 2, slab, size_x, size_y), jnp.bfloat16),
            pltpu.VMEM((slab, size_x, size_y), jnp.float32),
            pltpu.VMEM((slab * size_x, n_rec), jnp.bfloat16),
            pltpu.VMEM((slab * size_x, 2 * size_y), jnp.float32),
            pltpu.VMEM((3 * size_y, size_y), jnp.bfloat16),
            pltpu.VMEM((shot_n - 1, slab, size_x // shot_n, size_y), jnp.float32),
            pltpu.SemaphoreType.DMA((4,)),
            pltpu.SemaphoreType.DMA((ITERS, 2, shot_n)),
            pltpu.SemaphoreType.DMA((ITERS, 2, shot_n)),
            pltpu.SemaphoreType.DMA((3, shot_n - 1)),
            pltpu.SemaphoreType.DMA((3, shot_n - 1)),
        ],
        compiler_params=pltpu.CompilerParams(
            collective_id=0, has_side_effects=True, vmem_limit_bytes=60 * 1024 * 1024
        ),
    )(
        sources[0],
        spot,
        residual_traces[0],
        courant_sq,
        adjoint_init[0],
        forward_saved[0],
    )
    return gradient, final[None]


def solution(mesh):
    placed = (
        P(("groups", "dom"), None, None),
        P(("groups", "shot"), None, "dom", None, None),
        P(("groups", "shot"), None, "dom", None, None),
        P(("groups", "shot"), None, None),
        P(("groups", "shot"), None, None),
        P(("groups", "shot"), None),
    )
    return jax.shard_map(
        functools.partial(per_device, mesh.shape["dom"], mesh.shape["shot"]),
        mesh=mesh,
        in_specs=placed,
        out_specs=(
            P(("groups", "dom"), "shot", None),
            P(("groups", "shot"), None, "dom", None, None),
        ),
        check_vma=False,
    )
```
